32 devices in a mesh: groups: 2 (over y), seq: 16 (over z, x, core).
Axes of the slice: x: 2, y: 2, z: 4, core: 2. Of those that a mesh axis runs over, the one named last changes fastest.
Arguments:
- queries: bfloat16 [8192, 4096], P(('groups', 'seq')), parts along dimension 0, may hold values from -60 to 60
- vision: bfloat16 [512, 8192], P(('groups', 'seq')), parts along dimension 0, may hold values from -6 to 6
- w_key: bfloat16 [8192, 512], P('seq'), may hold values from -0.0625 to 0.0625
- w_value: bfloat16 [8192, 512], P('seq'), may hold values from -0.0625 to 0.0625
- key_gain: float32 [128], replicated, may hold values from 0.25 to 1.75
- image_range: int32 [8192, 2], P(('groups', 'seq')), parts along dimension 0, may hold values from 0 to 4, as said below
- image_counts: int32 [8], P('groups'), parts along dimension 0, may hold values from 32 to 64, as said below
Outputs:
- attended: bfloat16 [8192, 4096], P(('groups', 'seq')), parts along dimension 0
The draws below stay inside these ranges and needn't reach their ends.
There are 2 independent parts, one for each index of `groups`. The reference program is written for one: setup_inputs(seed, part) draws one part's arguments, and reference() takes and returns one part's arrays. A program takes and returns all parts, laid end to end along the dimension named above; an argument that names none is the same for every part. Nothing has to cross between parts.
Inputs may be any that keep to these rules, and one draw needn't show every extreme that they name: A text token attends to the last 1 to 3 images placed at or before its position; tokens before the first image attend to none (both ends 0); image_range[t, 1] never falls along t. `image_counts`: the valid tokens of an image are the first slots of its 64 slots; some image fills all of them.
All inputs are finite; a program needn't handle non-finite values.
Results may differ from the reference program's by a relative error of at most 0.012.
The reference program's roundings to bfloat16 on the way (of `keys`, `values` and `weights`) count: a program that leaves them out, or rounds other values in their place, can miss the bound.
Values may be sent and summed in bfloat16 or wider, within the bound.
A program may use at most 64 MiB of HBM per device.

```python
import math
import jax
import jax.numpy as jnp
from jax import lax

D = 8192
HD = 128
KV_HEADS = 4
HEADS = 32
GROUP = 8
IMAGES = 4
TOKENS = 4096
VISION = 256
SLOTS = 64


def draw_image_range(key, part):
    places = jnp.sort(jax.random.randint(jax.random.fold_in(key, 11), (IMAGES,), 0, TOKENS))
    span_sizes = jax.random.randint(jax.random.fold_in(key, 12), (IMAGES,), 1, 4)
    position = jnp.arange(TOKENS, dtype=jnp.int32)
    high_ends = jnp.sum((places[None, :] <= position[:, None]).astype(jnp.int32), axis=1)
    chosen = jnp.take(span_sizes, jnp.maximum(high_ends - 1, 0))
    low_ends = jnp.where(high_ends > 0, jnp.maximum(high_ends - chosen, 0), 0)
    return jnp.stack([low_ends, high_ends], axis=1).astype(jnp.int32)


def draw_image_counts(key, part):
    counts = jax.random.randint(jax.random.fold_in(key, 21), (IMAGES,), SLOTS // 2, SLOTS + 1)
    full_image = jax.random.randint(jax.random.fold_in(key, 22), (), 0, IMAGES)
    return jnp.where(jnp.arange(IMAGES) == full_image, SLOTS, counts).astype(jnp.int32)


def draw_queries(key, part):
    array_shape = (TOKENS, HEADS * HD)
    drawn = jnp.clip(jax.random.normal(jax.random.fold_in(key, 33), array_shape, jnp.float32), -6.0, 6.0)
    return drawn.astype(jnp.bfloat16)


def shard_levels(stream_key, shape, shards, least, top_value):
    def one(dim, parts):
        steps = jax.random.uniform(jax.random.fold_in(jax.random.fold_in(stream_key, 6), dim), (parts,), jnp.float32, least / len(shards), top_value / len(shards))
        return jnp.repeat(jnp.exp(steps), shape[dim] // parts).reshape((-1,) + (1,) * (len(shape) - dim - 1))

    factor_of = one(*shards[0])
    for cut in shards[1:]:
        factor_of = factor_of * one(*cut)
    return factor_of


def centred(stream_key, extent, deviation, bound, pieces=(), held_as=jnp.bfloat16):
    values = deviation * jax.random.normal(stream_key, extent, jnp.float32)
    if pieces:
        values = values * shard_levels(stream_key, extent, pieces, -0.22, 0.18)
    return jnp.clip(values, -bound, bound).astype(held_as)


def setup_inputs(seed: int = 0, part: int = 0) -> dict:
    keys = jax.random.split(jax.random.key(seed), 8)
    part_keys = jax.random.split(jax.random.fold_in(keys[7], part), 8)
    queries = draw_queries(jax.random.fold_in(jax.random.fold_in(keys[7], part), 71), part)
    vision = centred(part_keys[1], (VISION, D), 1.0, 6.0, ((0, 16),))
    w_key = centred(keys[2], (D, KV_HEADS * HD), D ** -0.5, 0.0625, ((0, 16),))
    w_value = centred(keys[3], (D, KV_HEADS * HD), D ** -0.5, 0.0625, ((0, 16),))
    key_gain = jnp.clip(1.0 + 0.15 * jax.random.normal(keys[4], (HD,), jnp.float32), 0.25, 1.75)
    image_range = draw_image_range(jax.random.fold_in(jax.random.fold_in(keys[7], part), 71), part)
    image_counts = draw_image_counts(jax.random.fold_in(jax.random.fold_in(keys[7], part), 71), part)
    return {"queries": queries, "vision": vision, "w_key": w_key, "w_value": w_value, "key_gain": key_gain, "image_range": image_range, "image_counts": image_counts}


def normed_keys(raw_keys, key_gain):
    head_view = raw_keys.reshape(raw_keys.shape[0], -1, key_gain.shape[0])
    inverse_rms = lax.rsqrt(lax.optimization_barrier(jnp.mean(head_view * head_view, axis=-1, keepdims=True)) + 1e-05)
    return (head_view * inverse_rms * key_gain).reshape(raw_keys.shape).astype(jnp.bfloat16)

def reference(queries, vision, w_key, w_value, key_gain, image_range, image_counts):
    key_raw = jnp.dot(vision, w_key, preferred_element_type=jnp.float32)
    value_raw = jnp.dot(vision, w_value, preferred_element_type=jnp.float32)
    key_rows = lax.optimization_barrier(normed_keys(key_raw, key_gain))
    value_rows = lax.optimization_barrier(value_raw.astype(jnp.bfloat16))
    key_heads = key_rows.astype(jnp.float32).reshape(VISION, KV_HEADS, HD)
    value_heads = value_rows.astype(jnp.float32).reshape(VISION, KV_HEADS, HD)
    indices = jnp.arange(VISION, dtype=jnp.int32)
    image_ids = indices // SLOTS
    slot_ids = indices - image_ids * SLOTS
    slot_live = slot_ids < jnp.take(image_counts, image_ids)
    block_rows = math.gcd(TOKENS, 512)
    blocks = TOKENS // block_rows

    def one_block(block_items):
        query_block, low_ends, high_ends = block_items
        query_view = query_block.astype(jnp.float32).reshape(block_rows, KV_HEADS, GROUP, HD)
        scores = jnp.einsum('tkgd,skd->tkgs', query_view, key_heads) / math.sqrt(HD)
        inside = (image_ids[None, :] >= low_ends[:, None]) & (image_ids[None, :] < high_ends[:, None])
        allowed_cube = (inside & slot_live[None, :])[:, None, None, :]
        row_max = lax.optimization_barrier(jnp.max(jnp.where(allowed_cube, scores, -1e+30), axis=-1, keepdims=True))
        shifted = jnp.where(allowed_cube, scores - row_max, 0.0)
        weights = jnp.where(allowed_cube, jnp.exp(shifted), 0.0).astype(jnp.bfloat16)
        weights = lax.optimization_barrier(weights).astype(jnp.float32)
        row_sum = lax.optimization_barrier(jnp.sum(weights, axis=-1))
        weighted = jnp.einsum('tkgs,skd->tkgd', weights, value_heads)
        result = weighted / jnp.where(row_sum > 0.0, row_sum, 1.0)[..., None]
        return result.reshape(block_rows, HEADS * HD).astype(jnp.bfloat16)
    outputs = lax.map(one_block, (queries.reshape(blocks, block_rows, HEADS * HD), image_range[:, 0].reshape(blocks, block_rows), image_range[:, 1].reshape(blocks, block_rows)))
    return outputs.reshape(TOKENS, HEADS * HD)
```

```python
import functools
import math

import jax
import jax.numpy as jnp
from jax import lax
from jax.experimental import pallas as pl
from jax.experimental.pallas import tpu as pltpu
from jax.sharding import PartitionSpec as P

MESH = pl.DeviceIdType.MESH
CORES = 2
CHUNKS = 1
STEPS = 2
DIRECT = (1,)
LINK = jnp.bfloat16


def normed_keys(raw_keys, gain):
    head_size = gain.shape[1]
    heads = []
    for start in range(0, raw_keys.shape[1], head_size):
        head = raw_keys[:, start : start + head_size]
        inverse_rms = lax.rsqrt(jnp.mean(head * head, axis=1, keepdims=True) + 1e-05)
        heads.append((head * inverse_rms * gain).astype(jnp.bfloat16))
    return jnp.concatenate(heads, axis=1)


def project_kernel(
    chips, vision_hbm, w_key_hbm, w_value_hbm, gain_ref, keys_hbm, values_hbm,
    vision, columns, w_both, partial, partial_k, key_sent, key_arrived, value_sent, value_arrived, rows_out,
    load_sem, weight_load_sem, weight_send_sem, weight_recv_sem,
    vision_send, vision_recv, partial_send, partial_recv,
    gather_send, gather_recv, pair_send, pair_recv, forward_send, forward_recv, out_sem,
):
    me = lax.axis_index("seq")
    group = lax.axis_index("groups")
    chip, core = me // CORES, me % CORES
    half, place, parity = chips // 2, chip // 2, chip % 2
    depth = w_key_hbm.shape[0]
    width = CORES * depth
    rows = columns.shape[2]
    partner = (group, chip * CORES + (1 - core))
    pair = (group, (place * 2 + 1 - parity) * CORES + core)
    peers = [lax.rem(chip + step, chips) for step in range(1, chips)]
    line = [lax.rem(place + step, half) * 2 + parity for step in range(1, half)]

    def at(chip_index):
        return (group, chip_index * CORES + core)

    load = pltpu.make_async_copy(vision_hbm, vision, load_sem)
    load.start()
    mine = pl.ds(pl.multiple_of(core * depth, depth), depth)
    weights = [w_key_hbm, w_value_hbm]
    weight_loads = [
        pltpu.make_async_copy(weights[i], w_both.at[i, mine], weight_load_sem.at[i]) for i in range(2)
    ]
    for copy in weight_loads:
        copy.start()

    barrier = pltpu.get_barrier_semaphore()
    for peer in peers:
        pl.semaphore_signal(barrier, inc=1, device_id=at(peer), device_id_type=MESH)
    pl.semaphore_signal(barrier, inc=1, device_id=partner, device_id_type=MESH)
    pl.semaphore_wait(barrier, chips)

    def remote(src, dst, send_sem, recv_sem, device):
        return pltpu.make_async_remote_copy(
            src_ref=src, dst_ref=dst, send_sem=send_sem, recv_sem=recv_sem,
            device_id=device, device_id_type=MESH,
        )

    load.wait()
    vision_copies = []
    for chunk in range(CHUNKS):
        own_rows = pl.ds(chunk * rows, rows)
        chunk_copies = []
        for step, peer in enumerate(peers):
            part = pl.ds(pl.multiple_of(peer * width, 128), width)
            copy = remote(
                vision.at[own_rows, part], columns.at[chunk, chip],
                vision_send.at[chunk, step], vision_recv.at[chunk, step], at(peer),
            )
            copy.start()
            chunk_copies.append(copy)
        vision_copies.append(chunk_copies)
    weight_sends = [
        remote(weights[i], w_both.at[i, mine], weight_send_sem.at[i], weight_recv_sem.at[i], partner)
        for i in range(2)
    ]
    for copy in weight_sends:
        copy.start()
    for chunk in range(CHUNKS):
        columns[chunk, chip] = vision[chunk * rows : (chunk + 1) * rows, pl.ds(pl.multiple_of(chip * width, 128), width)]
    for copy in weight_loads:
        copy.wait()
    for copy in weight_sends:
        copy.wait()

    streams = [(chunk, i) for chunk in range(CHUNKS) for i in range(2)]
    partial_copies = []
    for stream, (chunk, i) in enumerate(streams):
        if i == 0:
            for copy in vision_copies[chunk]:
                copy.wait()
        left = columns[chunk].reshape(chips * rows, width)
        product = jnp.dot(left, w_both[i], preferred_element_type=jnp.float32).reshape(chips, rows, -1)
        if i == 0:
            sent, landed = key_sent, key_arrived
            sent[chunk] = product.astype(sent.dtype)
            partial_k[...] = product
        else:
            sent, landed = value_sent, value_arrived
            sent[chunk] = product.astype(sent.dtype)
            partial[...] = product
        stream_copies = []
        for step, peer in enumerate(peers):
            copy = remote(
                sent.at[chunk, peer], landed.at[chunk, step],
                partial_send.at[stream, step], partial_recv.at[stream, step], at(peer),
            )
            copy.start()
            stream_copies.append(copy)
        if i == 0:
            own = None
        else:
            own = partial[chip]
        partial_copies.append((stream_copies, own))

    def block(stream, source):
        chunk, i = streams[stream]
        return rows_out.at[i, source, pl.ds(chunk * rows, rows)]

    def move(stream, source, send_sem, recv_sem, slot, device):
        ref = block(stream, source)
        copy = remote(ref, ref, send_sem.at[stream, slot], recv_sem.at[stream, slot], device)
        copy.start()
        return copy

    gathers, pairs, forwards = {}, {}, ([], [])

    def finish(stream):
        chunk, i = streams[stream]
        copies, total = partial_copies[stream]
        if i == 0:
            total = partial_k[chip]
        landed = key_arrived if i == 0 else value_arrived
        for step, copy in enumerate(copies):
            copy.wait()
            total = total + landed[chunk, step].astype(jnp.float32)
        done = normed_keys(total, gain_ref[...]) if i == 0 else total.astype(jnp.bfloat16)
        rows_out[i, me, chunk * rows : (chunk + 1) * rows] = done
        targets = peers if i in DIRECT else line
        gathers[stream] = [
            move(stream, me, gather_send, gather_recv, step, at(peer)) for step, peer in enumerate(targets)
        ]
        pairs[stream] = [] if i in DIRECT else [move(stream, me, pair_send, pair_recv, 0, pair)]
        forwards[streams[stream][1]].append(move(stream, me, forward_send, forward_recv, 0, partner))

    def pass_line(stream):
        chunk, i = streams[stream]
        for step, copy in enumerate(gathers[stream]):
            copy.wait()
            if i in DIRECT:
                source = lax.rem(chip + chips - 1 - step, chips) * CORES + core
            else:
                source = (lax.rem(place + half - 1 - step, half) * 2 + parity) * CORES + core
                pairs[stream].append(move(stream, source, pair_send, pair_recv, step + 1, pair))
            forwards[streams[stream][1]].append(move(stream, source, forward_send, forward_recv, step + 1, partner))

    def pass_pair(stream):
        for step, copy in enumerate(pairs[stream]):
            copy.wait()
            source = (lax.rem(place + half - step, half) * 2 + 1 - parity) * CORES + core
            forwards[streams[stream][1]].append(move(stream, source, forward_send, forward_recv, half + step, partner))

    count = len(streams)
    for turn in range(count + 2):
        for lag, act in enumerate((finish, pass_line, pass_pair)):
            if 0 <= turn - lag < count:
                act(turn - lag)
    outs = [
        pltpu.make_async_copy(rows_out.at[i], out, out_sem.at[i]) for i, out in enumerate([keys_hbm, values_hbm])
    ]
    for i in range(2):
        for copy in forwards[i]:
            copy.wait()
        outs[i].start()
    for copy in outs:
        copy.wait()


def project(vision, w_key, w_value, key_gain):
    shards = lax.axis_size("seq")
    chips = shards // CORES
    rows, full = vision.shape
    piece = rows // CHUNKS
    depth, kv_width = w_key.shape
    gathered = jax.ShapeDtypeStruct((shards, rows, kv_width), jnp.bfloat16)
    dma = pltpu.SemaphoreType.DMA
    hops, half, streams = chips - 1, chips // 2, 2 * CHUNKS
    f32, bf16 = jnp.float32, jnp.bfloat16
    keys, values = pl.pallas_call(
        functools.partial(project_kernel, chips),
        out_shape=(gathered, gathered),
        in_specs=[pl.BlockSpec(memory_space=pl.ANY)] * 3 + [pl.BlockSpec(memory_space=pltpu.VMEM)],
        out_specs=(pl.BlockSpec(memory_space=pl.ANY),) * 2,
        scratch_shapes=[
            pltpu.VMEM((rows, full), bf16),
            pltpu.VMEM((CHUNKS, chips, piece, CORES * depth), bf16),
            pltpu.VMEM((2, CORES * depth, kv_width), bf16),
            pltpu.VMEM((chips, piece, kv_width), f32),
            pltpu.VMEM((chips, piece, kv_width), f32),
            pltpu.VMEM((CHUNKS, chips, piece, kv_width), LINK),
            pltpu.VMEM((CHUNKS, hops, piece, kv_width), LINK),
            pltpu.VMEM((CHUNKS, chips, piece, kv_width), LINK),
            pltpu.VMEM((CHUNKS, hops, piece, kv_width), LINK),
            pltpu.VMEM((2, shards, rows, kv_width), bf16),
            dma, dma((2,)), dma((2,)), dma((2,)),
            dma((CHUNKS, hops)), dma((CHUNKS, hops)), dma((streams, hops)), dma((streams, hops)),
            dma((streams, hops)), dma((streams, hops)),
            dma((streams, half)), dma((streams, half)),
            dma((streams, chips)), dma((streams, chips)), dma((2,)),
        ],
        compiler_params=pltpu.CompilerParams(collective_id=0, has_side_effects=True),
        name="project",
    )(vision, w_key, w_value, key_gain.reshape(1, -1))
    return keys.reshape(shards * rows, kv_width), values.reshape(shards * rows, kv_width)


def attend_kernel(slot_count, head_size, counts_ref, range_ref, queries_ref, keys_ref, values_ref, out_ref, bias):
    vision_rows = keys_ref.shape[0]

    @pl.when(pl.program_id(0) == 0)
    def _():
        low_ends, high_ends = range_ref[0:1, :], range_ref[1:2, :]
        index = lax.broadcasted_iota(jnp.int32, (vision_rows, 1), 0)
        image = jnp.zeros_like(index)
        first = jnp.zeros_like(index)
        limit = jnp.zeros_like(index) + counts_ref[0]
        for i in range(1, counts_ref.shape[0]):
            past = index >= i * slot_count
            image = jnp.where(past, i, image)
            first = jnp.where(past, i * slot_count, first)
            limit = jnp.where(past, counts_ref[i], limit)
        live_image = jnp.where(index - first < limit, image, -1)
        allowed = (live_image >= low_ends) & (live_image < high_ends)
        bias[...] = jnp.where(allowed, 0.0, -1e30).T

    scale = math.log2(math.e) / math.sqrt(head_size)
    kv_block = keys_ref.shape[1] // head_size
    group_width = queries_ref.shape[1] // kv_block
    ones = jnp.ones((vision_rows, head_size), jnp.bfloat16)
    for kv_head in range(kv_block):
        kv_part = pl.ds(kv_head * head_size, head_size)
        keys = keys_ref[:, kv_part]
        values = jnp.concatenate([values_ref[:, kv_part], ones], axis=1)
        for start in range(kv_head * group_width, (kv_head + 1) * group_width, head_size):
            head = pl.ds(start, head_size)
            scores = lax.dot_general(
                queries_ref[:, head], keys, (((1,), (1,)), ((), ())), preferred_element_type=jnp.float32
            )
            scores = scores + bias[...]
            row_max = jnp.maximum(jnp.max(scores, axis=1, keepdims=True), -1e29)
            weights = jnp.exp2((scores - row_max) * scale).astype(jnp.bfloat16)
            summed = jnp.dot(weights, values, preferred_element_type=jnp.float32)
            weighted, row_sum = summed[:, :head_size], summed[:, head_size:]
            out_ref[:, head] = (weighted / jnp.where(row_sum > 0.0, row_sum, 1.0)).astype(jnp.bfloat16)


def attend(queries, keys, values, image_range, image_counts, head_size):
    tokens, query_width = queries.shape
    vision_rows, kv_width = keys.shape
    kv_heads = kv_width // head_size
    steps = math.gcd(kv_heads, STEPS)
    group_width = query_width // steps
    kv_block = kv_width // steps
    slot_count = vision_rows // image_counts.shape[0]
    return pl.pallas_call(
        functools.partial(attend_kernel, slot_count, head_size),
        out_shape=jax.ShapeDtypeStruct(queries.shape, jnp.bfloat16),
        grid=(steps,),
        in_specs=[
            pl.BlockSpec(memory_space=pltpu.SMEM),
            pl.BlockSpec((2, tokens), lambda h: (0, 0)),
            pl.BlockSpec((tokens, group_width), lambda h: (0, h)),
            pl.BlockSpec((vision_rows, kv_block), lambda h: (0, h)),
            pl.BlockSpec((vision_rows, kv_block), lambda h: (0, h)),
        ],
        out_specs=pl.BlockSpec((tokens, group_width), lambda h: (0, h)),
        scratch_shapes=[pltpu.VMEM((tokens, vision_rows), jnp.float32)],
        name="attend",
    )(image_counts, image_range.T, queries, keys, values)


def per_device(queries, vision, w_key, w_value, key_gain, image_range, image_counts):
    keys, values = project(vision, w_key, w_value, key_gain)
    return attend(queries, keys, values, image_range, image_counts, key_gain.shape[0])


def solution(mesh):
    placed = (
        P(("groups", "seq"), None),
        P(("groups", "seq"), None),
        P("seq", None),
        P("seq", None),
        P(),
        P(("groups", "seq"), None),
        P("groups"),
    )
    return jax.shard_map(
        per_device,
        mesh=mesh,
        in_specs=placed,
        out_specs=P(("groups", "seq"), None),
        check_vma=False,
    )
```

```python
import functools
import math

import jax
import jax.numpy as jnp
from jax import lax
from jax.experimental import pallas as pl
from jax.experimental.pallas import tpu as pltpu
from jax.sharding import PartitionSpec as P

MESH = pl.DeviceIdType.MESH
CORES = 2
STEPS = 2
STORE_HEADS = 4
EARLY_HEADS = 24
LINK = jnp.bfloat16
MASKED = -1e30
MIB = 1024 * 1024
WEIGHTS_MAX = 8 * MIB


def normed_keys(raw_keys, gain):
    head_size = gain.shape[1]
    heads = []
    for start in range(0, raw_keys.shape[1], head_size):
        head = raw_keys[:, start : start + head_size]
        inverse_rms = lax.rsqrt(jnp.mean(head * head, axis=1, keepdims=True) + 1e-05)
        heads.append((head * inverse_rms * gain).astype(jnp.bfloat16))
    return jnp.concatenate(heads, axis=1)


def token_marks(range_ref, images, width):
    low_ends, high_ends = range_ref[0:1, :], range_ref[1:2, :]
    image = lax.broadcasted_iota(jnp.int32, (width, 1), 0)
    outside = (image < low_ends) | (image >= high_ends)
    marked = ((image < images) & outside) | (image == images)
    return jnp.where(marked, 1.0, 0.0).T.astype(jnp.bfloat16)


def row_marks(counts_ref, vision_rows, width):
    images = counts_ref.shape[0]
    slot_count = vision_rows // images
    index = lax.broadcasted_iota(jnp.int32, (vision_rows, width), 0)
    column = lax.broadcasted_iota(jnp.int32, (vision_rows, width), 1)
    image = jnp.zeros_like(index)
    first = jnp.zeros_like(index)
    limit = jnp.zeros_like(index) + counts_ref[0]
    for i in range(1, images):
        past = index >= i * slot_count
        image = jnp.where(past, i, image)
        first = jnp.where(past, i * slot_count, first)
        limit = jnp.where(past, counts_ref[i], limit)
    dead = index - first >= limit
    return jnp.where((column == image) | ((column == images) & dead), MASKED, 0.0).astype(jnp.bfloat16)


def project_kernel(chips, fused, *refs):
    if fused:
        vision_hbm, w_key_hbm, w_value_hbm, gain_hbm, counts_hbm, range_hbm, queries_hbm = refs[:7]
        weights_ref, values_ref = refs[7:9]
        counts_ref, range_ref, queries, marks, row_mark, extra_sem = refs[9:15]
        refs = refs[15:]
    else:
        vision_hbm, w_key_hbm, w_value_hbm, gain_hbm, keys_ref, values_ref = refs[:6]
        refs = refs[6:]
    (
        gain_ref, gain_sem, vision, columns, w_both, partial, sent, arrived, gathered,
        load_sem, weight_load_sem, weight_send_sem, weight_recv_sem, vision_send, vision_recv,
        partial_send, partial_recv, gather_send, gather_recv, forward_send, forward_recv,
    ) = refs
    me = lax.axis_index("seq")
    group = lax.axis_index("groups")
    chip, core = me // CORES, me % CORES
    depth = w_key_hbm.shape[0]
    width = CORES * depth
    rows = columns.shape[1]
    partner = (group, chip * CORES + (1 - core))
    peers = [lax.rem(chip + step, chips) for step in range(1, chips)]

    def at(chip_index):
        return (group, chip_index * CORES + core)

    load = pltpu.make_async_copy(vision_hbm, vision, load_sem)
    load.start()
    mine = pl.ds(pl.multiple_of(core * depth, depth), depth)
    weights = [w_key_hbm, w_value_hbm]
    weight_loads = [
        pltpu.make_async_copy(weights[i], w_both.at[i, mine], weight_load_sem.at[i]) for i in range(2)
    ]
    for copy in weight_loads:
        copy.start()
    gain_load = pltpu.make_async_copy(gain_hbm, gain_ref, gain_sem)
    gain_load.start()
    if fused:
        counts_load, range_load, query_load = [
            pltpu.make_async_copy(source, target, extra_sem.at[i])
            for i, (source, target) in enumerate(
                [(counts_hbm, counts_ref), (range_hbm, range_ref), (queries_hbm, queries)]
            )
        ]
        counts_load.start()
        range_load.start()
        query_load.start()

    barrier = pltpu.get_barrier_semaphore()
    for peer in peers:
        pl.semaphore_signal(barrier, inc=1, device_id=at(peer), device_id_type=MESH)
    pl.semaphore_signal(barrier, inc=1, device_id=partner, device_id_type=MESH)
    pl.semaphore_wait(barrier, chips)

    def remote(src, dst, send_sem, recv_sem, device):
        return pltpu.make_async_remote_copy(
            src_ref=src, dst_ref=dst, send_sem=send_sem, recv_sem=recv_sem,
            device_id=device, device_id_type=MESH,
        )

    load.wait()
    vision_copies = []
    for step, peer in enumerate(peers):
        part = pl.ds(pl.multiple_of(peer * width, 128), width)
        copy = remote(vision.at[:, part], columns.at[chip], vision_send.at[step], vision_recv.at[step], at(peer))
        copy.start()
        vision_copies.append(copy)
    for copy in weight_loads:
        copy.wait()
    weight_sends = [
        remote(w_both.at[i, mine], w_both.at[i, mine], weight_send_sem.at[i], weight_recv_sem.at[i], partner)
        for i in range(2)
    ]
    for copy in weight_sends:
        copy.start()
    columns[chip] = vision[:, pl.ds(pl.multiple_of(chip * width, 128), width)]
    gain_load.wait()
    if fused:
        counts_load.wait()
        range_load.wait()
        marks[...] = token_marks(range_ref, counts_ref.shape[0], marks.shape[1])
        row_mark[...] = row_marks(counts_ref, *row_mark.shape)
    for copy in weight_sends:
        copy.wait()
    for copy in vision_copies:
        copy.wait()

    partial_copies = []
    for i in range(2):
        left = columns[...].reshape(chips * rows, width)
        product = jnp.dot(left, w_both[i], preferred_element_type=jnp.float32).reshape(chips, rows, -1)
        sent[i] = product.astype(sent.dtype)
        partial[...] = product
        stream_copies = []
        for step, peer in enumerate(peers):
            copy = remote(
                sent.at[i, peer], arrived.at[i, step], partial_send.at[i, step], partial_recv.at[i, step], at(peer),
            )
            copy.start()
            stream_copies.append(copy)
        partial_copies.append((stream_copies, partial[chip]))

    def forward(i, source, slot):
        ref = gathered.at[i, source]
        copy = remote(ref, ref, forward_send.at[i, slot], forward_recv.at[i, slot], partner)
        copy.start()
        return copy

    gathers, forwards = [], ([], [])
    for i in range(2):
        copies, total = partial_copies[i]
        for step, copy in enumerate(copies):
            copy.wait()
            total = total + arrived[i, step].astype(jnp.float32)
        done = normed_keys(total, gain_ref[...]) if i == 0 else total.astype(jnp.bfloat16)
        gathered[i, me] = done
        ref = gathered.at[i, me]
        stream_copies = []
        for step, peer in enumerate(peers):
            copy = remote(ref, ref, gather_send.at[i, step], gather_recv.at[i, step], at(peer))
            copy.start()
            stream_copies.append(copy)
        gathers.append(stream_copies)
        forwards[i].append(forward(i, me, 0))

    def pass_on(i):
        for step, copy in enumerate(gathers[i]):
            copy.wait()
            source = lax.rem(chip + chips - 1 - step, chips) * CORES + core
            forwards[i].append(forward(i, source, step + 1))

    def settle(i):
        for copy in forwards[i]:
            copy.wait()

    pass_on(0)
    settle(0)
    if fused:
        query_load.wait()
        head_size = gain_ref.shape[1]
        heads = weights_ref.shape[0]
        group_size = heads // (gathered.shape[3] // head_size)
        scale = math.log2(math.e) / math.sqrt(head_size)

        def weigh(head):
            start = head // group_size * head_size
            keys = gathered[0, :, :, start : start + head_size].reshape(-1, head_size)
            keys = jnp.concatenate([keys, row_mark[...]], axis=1)
            marked = jnp.concatenate([queries[:, head * head_size : (head + 1) * head_size], marks[...]], axis=1)
            scores = lax.dot_general(marked, keys, (((1,), (1,)), ((), ())), preferred_element_type=jnp.float32)
            row_max = jnp.maximum(jnp.max(scores, axis=1, keepdims=True), -1e29)
            weights_ref[head] = jnp.exp2((scores - row_max) * scale).astype(jnp.bfloat16)

        early = min(EARLY_HEADS, heads)
        for head in range(early):
            weigh(head)
        pass_on(1)
        for head in range(early, heads):
            weigh(head)
    else:
        pass_on(1)
        keys_ref[...] = gathered[0]
    settle(1)
    values_ref[...] = gathered[1]


def project(vision, w_key, w_value, key_gain, extra):
    shards = lax.axis_size("seq")
    chips = shards // CORES
    rows, full = vision.shape
    depth, kv_width = w_key.shape
    head_size = key_gain.shape[0]
    fused = bool(extra)
    block = jax.ShapeDtypeStruct((shards, rows, kv_width), jnp.bfloat16)
    dma = pltpu.SemaphoreType.DMA
    hops = chips - 1
    f32, bf16 = jnp.float32, jnp.bfloat16
    hbm, vmem = pl.BlockSpec(memory_space=pltpu.HBM), pl.BlockSpec(memory_space=pltpu.VMEM)
    inputs = (vision, w_key, w_value, key_gain.reshape(1, -1), *extra)
    extra_scratch = []
    first = block
    if fused:
        tokens, query_width = extra[2].shape
        first = jax.ShapeDtypeStruct((query_width // head_size, tokens, shards * rows), bf16)
        extra_scratch = [
            pltpu.SMEM(extra[0].shape, jnp.int32),
            pltpu.VMEM(extra[1].shape, jnp.int32),
            pltpu.VMEM((tokens, query_width), bf16),
            pltpu.VMEM((tokens, head_size), bf16),
            pltpu.VMEM((shards * rows, head_size), bf16),
            dma((3,)),
        ]
    return pl.pallas_call(
        functools.partial(project_kernel, chips, fused),
        out_shape=(first, block),
        in_specs=[hbm] * len(inputs),
        out_specs=(vmem, vmem),
        scratch_shapes=[
            *extra_scratch,
            pltpu.VMEM((1, head_size), f32),
            dma,
            pltpu.VMEM((rows, full), bf16),
            pltpu.VMEM((chips, rows, CORES * depth), bf16),
            pltpu.VMEM((2, CORES * depth, kv_width), bf16),
            pltpu.VMEM((chips, rows, kv_width), f32),
            pltpu.VMEM((2, chips, rows, kv_width), LINK),
            pltpu.VMEM((2, hops, rows, kv_width), LINK),
            pltpu.VMEM((2, shards, rows, kv_width), bf16),
            dma, dma((2,)), dma((2,)), dma((2,)), dma((hops,)), dma((hops,)),
            dma((2, hops)), dma((2, hops)), dma((2, hops)), dma((2, hops)), dma((2, chips)), dma((2, chips)),
        ],
        compiler_params=pltpu.CompilerParams(
            collective_id=0, has_side_effects=True, vmem_limit_bytes=24 * MIB
        ),
        name="project",
    )(*[pltpu.with_memory_space_constraint(each, pltpu.HBM) for each in inputs])


def mix_kernel(head_size, weights_ref, values_ref, out_hbm, mixed, out_sem):
    heads, _, vision_rows = weights_ref.shape
    kv_heads = values_ref.shape[1] // head_size
    group_size = heads // kv_heads
    ones = jnp.ones((vision_rows, head_size), jnp.bfloat16)
    stores = []
    for head in range(heads):
        start = head // group_size * head_size
        values = jnp.concatenate([values_ref[:, start : start + head_size], ones], axis=1)
        summed = jnp.dot(weights_ref[head], values, preferred_element_type=jnp.float32)
        weighted, row_sum = summed[:, :head_size], summed[:, head_size:]
        mixed[:, head * head_size : (head + 1) * head_size] = (
            weighted / jnp.maximum(row_sum, 1.0)
        ).astype(jnp.bfloat16)
        if (head + 1) % STORE_HEADS == 0 or head + 1 == heads:
            first = head // STORE_HEADS * STORE_HEADS
            part = pl.ds(first * head_size, (head + 1 - first) * head_size)
            store = pltpu.make_async_copy(mixed.at[:, part], out_hbm.at[:, part], out_sem.at[len(stores)])
            store.start()
            stores.append(store)
    for store in stores:
        store.wait()


def mix(weights, values, head_size):
    heads, tokens, _ = weights.shape
    vmem = pl.BlockSpec(memory_space=pltpu.VMEM)
    return pl.pallas_call(
        functools.partial(mix_kernel, head_size),
        out_shape=jax.ShapeDtypeStruct((tokens, heads * head_size), jnp.bfloat16),
        in_specs=[vmem, vmem],
        out_specs=pl.BlockSpec(memory_space=pl.ANY),
        scratch_shapes=[
            pltpu.VMEM((tokens, heads * head_size), jnp.bfloat16),
            pltpu.SemaphoreType.DMA((pl.cdiv(heads, STORE_HEADS),)),
        ],
        compiler_params=pltpu.CompilerParams(vmem_limit_bytes=16 * MIB),
        name="mix",
    )(weights, values)


def attend_kernel(head_size, counts_ref, range_ref, queries_ref, keys_ref, values_ref, out_ref, marks, row_mark):
    vision_rows = keys_ref.shape[0]

    @pl.when(pl.program_id(0) == 0)
    def _():
        marks[...] = token_marks(range_ref, counts_ref.shape[0], head_size)
        row_mark[...] = row_marks(counts_ref, vision_rows, head_size)

    scale = math.log2(math.e) / math.sqrt(head_size)
    kv_block = keys_ref.shape[1] // head_size
    group_width = queries_ref.shape[1] // kv_block
    ones = jnp.ones((vision_rows, head_size), jnp.bfloat16)
    for kv_head in range(kv_block):
        kv_part = pl.ds(kv_head * head_size, head_size)
        keys = jnp.concatenate([keys_ref[:, kv_part], row_mark[...]], axis=1)
        values = jnp.concatenate([values_ref[:, kv_part], ones], axis=1)
        for start in range(kv_head * group_width, (kv_head + 1) * group_width, head_size):
            head = pl.ds(start, head_size)
            marked = jnp.concatenate([queries_ref[:, head], marks[...]], axis=1)
            scores = lax.dot_general(marked, keys, (((1,), (1,)), ((), ())), preferred_element_type=jnp.float32)
            row_max = jnp.maximum(jnp.max(scores, axis=1, keepdims=True), -1e29)
            weights = jnp.exp2((scores - row_max) * scale).astype(jnp.bfloat16)
            summed = jnp.dot(weights, values, preferred_element_type=jnp.float32)
            weighted, row_sum = summed[:, :head_size], summed[:, head_size:]
            out_ref[:, head] = (weighted / jnp.maximum(row_sum, 1.0)).astype(jnp.bfloat16)


def attend(queries, keys, values, image_range, image_counts, head_size):
    tokens, query_width = queries.shape
    vision_rows, kv_width = keys.shape
    steps = math.gcd(kv_width // head_size, STEPS)
    group_width = query_width // steps
    kv_block = kv_width // steps
    return pl.pallas_call(
        functools.partial(attend_kernel, head_size),
        out_shape=jax.ShapeDtypeStruct(queries.shape, jnp.bfloat16),
        grid=(steps,),
        in_specs=[
            pl.BlockSpec(memory_space=pltpu.SMEM),
            pl.BlockSpec((2, tokens), lambda h: (0, 0)),
            pl.BlockSpec((tokens, group_width), lambda h: (0, h)),
            pl.BlockSpec((vision_rows, kv_block), lambda h: (0, h)),
            pl.BlockSpec((vision_rows, kv_block), lambda h: (0, h)),
        ],
        out_specs=pl.BlockSpec((tokens, group_width), lambda h: (0, h)),
        scratch_shapes=[
            pltpu.VMEM((tokens, head_size), jnp.bfloat16),
            pltpu.VMEM((vision_rows, head_size), jnp.bfloat16),
        ],
        name="attend",
    )(image_counts, image_range.T, queries, keys, values)


def per_device(queries, vision, w_key, w_value, key_gain, image_range, image_counts):
    head_size = key_gain.shape[0]
    tokens, query_width = queries.shape
    vision_rows = vision.shape[0] * lax.axis_size("seq")
    weight_bytes = query_width // head_size * tokens * vision_rows * 2
    fused = weight_bytes <= WEIGHTS_MAX
    extra = (image_counts, image_range.T, queries) if fused else ()
    first, values = project(vision, w_key, w_value, key_gain, extra)
    values = values.reshape(vision_rows, -1)
    if fused:
        return mix(first, values, head_size)
    return attend(queries, first.reshape(vision_rows, -1), values, image_range, image_counts, head_size)


def solution(mesh):
    placed = (
        P(("groups", "seq"), None),
        P(("groups", "seq"), None),
        P("seq", None),
        P("seq", None),
        P(),
        P(("groups", "seq"), None),
        P("groups"),
    )
    return jax.shard_map(
        per_device,
        mesh=mesh,
        in_specs=placed,
        out_specs=P(("groups", "seq"), None),
        check_vma=False,
    )
```

```python
import functools
import math

import jax
import jax.numpy as jnp
from jax import lax
from jax.experimental import pallas as pl
from jax.experimental.pallas import tpu as pltpu
from jax.sharding import PartitionSpec as P

MESH = pl.DeviceIdType.MESH
CORES = 2
STEPS = 2
STORE_HEADS = 4
EARLY_HEADS = 24
LINK = jnp.bfloat16
MASKED = -1e30
MIB = 1024 * 1024
WEIGHTS_MAX = 8 * MIB


def normed_keys(raw_keys, gain):
    head_size = gain.shape[1]
    heads = []
    for start in range(0, raw_keys.shape[1], head_size):
        head = raw_keys[:, start : start + head_size]
        inverse_rms = lax.rsqrt(jnp.mean(head * head, axis=1, keepdims=True) + 1e-05)
        heads.append((head * inverse_rms * gain).astype(jnp.bfloat16))
    return jnp.concatenate(heads, axis=1)


def token_marks(range_ref, images, width):
    low_ends, high_ends = range_ref[0:1, :], range_ref[1:2, :]
    image = lax.broadcasted_iota(jnp.int32, (width, 1), 0)
    outside = (image < low_ends) | (image >= high_ends)
    marked = ((image < images) & outside) | (image == images)
    return jnp.where(marked, 1.0, 0.0).T.astype(jnp.bfloat16)


def row_marks(counts_ref, vision_rows, width):
    images = counts_ref.shape[0]
    slot_count = vision_rows // images
    index = lax.broadcasted_iota(jnp.int32, (vision_rows, width), 0)
    column = lax.broadcasted_iota(jnp.int32, (vision_rows, width), 1)
    image = jnp.zeros_like(index)
    first = jnp.zeros_like(index)
    limit = jnp.zeros_like(index) + counts_ref[0]
    for i in range(1, images):
        past = index >= i * slot_count
        image = jnp.where(past, i, image)
        first = jnp.where(past, i * slot_count, first)
        limit = jnp.where(past, counts_ref[i], limit)
    dead = index - first >= limit
    return jnp.where((column == image) | ((column == images) & dead), MASKED, 0.0).astype(jnp.bfloat16)


def project_kernel(chips, fused, *refs):
    if fused:
        vision_hbm, w_key_hbm, w_value_hbm, gain_hbm, counts_hbm, range_hbm, queries_hbm = refs[:7]
        weights_ref, values_ref = refs[7:9]
        counts_ref, range_ref, queries, marks, row_mark, extra_sem = refs[9:15]
        refs = refs[15:]
    else:
        vision_hbm, w_key_hbm, w_value_hbm, gain_hbm, keys_ref, values_ref = refs[:6]
        refs = refs[6:]
    (
        gain_ref, gain_sem, vision, columns, w_both, partial, sent, arrived, gathered,
        load_sem, weight_load_sem, weight_send_sem, weight_recv_sem, vision_send, vision_recv,
        partial_send, partial_recv, gather_send, gather_recv, forward_send, forward_recv,
    ) = refs
    me = lax.axis_index("seq")
    group = lax.axis_index("groups")
    chip, core = me // CORES, me % CORES
    depth = w_key_hbm.shape[0]
    width = CORES * depth
    rows = columns.shape[1]
    partner = (group, chip * CORES + (1 - core))
    hops = chips - 1
    peers = [lax.rem(chip + step, chips) for step in range(1, chips)]
    sources = [lax.rem(chip + chips - step, chips) for step in range(1, chips)]

    def at(chip_index):
        return (group, chip_index * CORES + core)

    load = pltpu.make_async_copy(vision_hbm, vision, load_sem)
    load.start()
    mine = pl.ds(pl.multiple_of(core * depth, depth), depth)
    weights = [w_key_hbm, w_value_hbm]
    weight_loads = [
        pltpu.make_async_copy(weights[i], w_both.at[i, mine], weight_load_sem.at[i]) for i in range(2)
    ]
    for copy in weight_loads:
        copy.start()
    gain_load = pltpu.make_async_copy(gain_hbm, gain_ref, gain_sem)
    gain_load.start()
    if fused:
        counts_load, range_load, query_load = [
            pltpu.make_async_copy(source, target, extra_sem.at[i])
            for i, (source, target) in enumerate(
                [(counts_hbm, counts_ref), (range_hbm, range_ref), (queries_hbm, queries)]
            )
        ]
        counts_load.start()
        range_load.start()
        query_load.start()

    barrier = pltpu.get_barrier_semaphore()
    for peer in peers:
        pl.semaphore_signal(barrier, inc=1, device_id=at(peer), device_id_type=MESH)
    pl.semaphore_signal(barrier, inc=1, device_id=partner, device_id_type=MESH)
    pl.semaphore_wait(barrier, chips)

    def remote(src, dst, send_sem, recv_sem, device):
        return pltpu.make_async_remote_copy(
            src_ref=src, dst_ref=dst, send_sem=send_sem, recv_sem=recv_sem,
            device_id=device, device_id_type=MESH,
        )

    load.wait()
    vision_copies = []
    for step, peer in reversed(list(enumerate(peers))):
        part = pl.ds(pl.multiple_of(peer * width, 128), width)
        copy = remote(vision.at[:, part], columns.at[step], vision_send.at[step], vision_recv.at[step], at(peer))
        copy.start()
        vision_copies.append(copy)
    for copy in weight_loads:
        copy.wait()
    weight_sends = [
        remote(w_both.at[i, mine], w_both.at[i, mine], weight_send_sem.at[i], weight_recv_sem.at[i], partner)
        for i in range(2)
    ]
    for copy in weight_sends:
        copy.start()
    columns[hops] = vision[:, pl.ds(pl.multiple_of(chip * width, 128), width)]
    gain_load.wait()
    if fused:
        counts_load.wait()
        range_load.wait()
        marks[...] = token_marks(range_ref, counts_ref.shape[0], marks.shape[1])
        row_mark[...] = row_marks(counts_ref, *row_mark.shape)
    for copy in weight_sends:
        copy.wait()

    for copy in vision_copies:
        copy.wait()

    partial_copies = ([], [])
    for i in range(2):
        left = columns[...].reshape(chips * rows, width)
        product = jnp.dot(left, w_both[i], preferred_element_type=jnp.float32).reshape(chips, rows, -1)
        sent[i] = product[:hops].astype(sent.dtype)
        partial[i] = product[hops]
        for step in range(hops):
            copy = remote(
                sent.at[i, step], arrived.at[i, step], partial_send.at[i, step], partial_recv.at[i, step],
                at(sources[step]),
            )
            copy.start()
            partial_copies[i].append(copy)

    def forward(i, source, slot):
        ref = gathered.at[i, source]
        copy = remote(ref, ref, forward_send.at[i, slot], forward_recv.at[i, slot], partner)
        copy.start()
        return copy

    gathers, forwards = [], ([], [])
    for i in range(2):
        total = partial[i]
        for step, copy in enumerate(partial_copies[i]):
            copy.wait()
            total = total + arrived[i, step].astype(jnp.float32)
        done = normed_keys(total, gain_ref[...]) if i == 0 else total.astype(jnp.bfloat16)
        gathered[i, me] = done
        ref = gathered.at[i, me]
        stream_copies = []
        for step, peer in enumerate(peers):
            copy = remote(ref, ref, gather_send.at[i, step], gather_recv.at[i, step], at(peer))
            copy.start()
            stream_copies.append(copy)
        gathers.append(stream_copies)
        forwards[i].append(forward(i, me, 0))

    def pass_on(i):
        for step in reversed(range(hops)):
            gathers[i][step].wait()
            source = sources[step] * CORES + core
            forwards[i].append(forward(i, source, step + 1))

    def settle(i):
        for copy in forwards[i]:
            copy.wait()

    pass_on(0)
    settle(0)
    if fused:
        query_load.wait()
        head_size = gain_ref.shape[1]
        heads = weights_ref.shape[0]
        group_size = heads // (gathered.shape[3] // head_size)
        scale = math.log2(math.e) / math.sqrt(head_size)

        def weigh(head):
            start = head // group_size * head_size
            keys = gathered[0, :, :, start : start + head_size].reshape(-1, head_size)
            keys = jnp.concatenate([keys, row_mark[...]], axis=1)
            marked = jnp.concatenate([queries[:, head * head_size : (head + 1) * head_size], marks[...]], axis=1)
            scores = lax.dot_general(marked, keys, (((1,), (1,)), ((), ())), preferred_element_type=jnp.float32)
            row_max = jnp.maximum(jnp.max(scores, axis=1, keepdims=True), -1e29)
            weights_ref[head] = jnp.exp2((scores - row_max) * scale).astype(jnp.bfloat16)

        early = min(EARLY_HEADS, heads)
        for head in range(early):
            weigh(head)
        pass_on(1)
        for head in range(early, heads):
            weigh(head)
    else:
        pass_on(1)
        keys_ref[...] = gathered[0]
    settle(1)
    values_ref[...] = gathered[1]


def project(vision, w_key, w_value, key_gain, extra):
    shards = lax.axis_size("seq")
    chips = shards // CORES
    rows, full = vision.shape
    depth, kv_width = w_key.shape
    head_size = key_gain.shape[0]
    fused = bool(extra)
    block = jax.ShapeDtypeStruct((shards, rows, kv_width), jnp.bfloat16)
    dma = pltpu.SemaphoreType.DMA
    hops = chips - 1
    f32, bf16 = jnp.float32, jnp.bfloat16
    hbm, vmem = pl.BlockSpec(memory_space=pltpu.HBM), pl.BlockSpec(memory_space=pltpu.VMEM)
    inputs = (vision, w_key, w_value, key_gain.reshape(1, -1), *extra)
    extra_scratch = []
    first = block
    if fused:
        tokens, query_width = extra[2].shape
        first = jax.ShapeDtypeStruct((query_width // head_size, tokens, shards * rows), bf16)
        extra_scratch = [
            pltpu.SMEM(extra[0].shape, jnp.int32),
            pltpu.VMEM(extra[1].shape, jnp.int32),
            pltpu.VMEM((tokens, query_width), bf16),
            pltpu.VMEM((tokens, head_size), bf16),
            pltpu.VMEM((shards * rows, head_size), bf16),
            dma((3,)),
        ]
    return pl.pallas_call(
        functools.partial(project_kernel, chips, fused),
        out_shape=(first, block),
        in_specs=[hbm] * len(inputs),
        out_specs=(vmem, vmem),
        scratch_shapes=[
            *extra_scratch,
            pltpu.VMEM((1, head_size), f32),
            dma,
            pltpu.VMEM((rows, full), bf16),
            pltpu.VMEM((chips, rows, CORES * depth), bf16),
            pltpu.VMEM((2, CORES * depth, kv_width), bf16),
            pltpu.VMEM((2, rows, kv_width), f32),
            pltpu.VMEM((2, hops, rows, kv_width), LINK),
            pltpu.VMEM((2, hops, rows, kv_width), LINK),
            pltpu.VMEM((2, shards, rows, kv_width), bf16),
            dma, dma((2,)), dma((2,)), dma((2,)), dma((hops,)), dma((hops,)),
            dma((2, hops)), dma((2, hops)), dma((2, hops)), dma((2, hops)), dma((2, chips)), dma((2, chips)),
        ],
        compiler_params=pltpu.CompilerParams(
            collective_id=0, has_side_effects=True, vmem_limit_bytes=24 * MIB
        ),
        name="project",
    )(*[pltpu.with_memory_space_constraint(each, pltpu.HBM) for each in inputs])


def mix_kernel(head_size, weights_ref, values_ref, out_hbm, mixed, out_sem):
    heads, _, vision_rows = weights_ref.shape
    kv_heads = values_ref.shape[1] // head_size
    group_size = heads // kv_heads
    ones = jnp.ones((vision_rows, head_size), jnp.bfloat16)
    stores = []
    for head in range(heads):
        start = head // group_size * head_size
        values = jnp.concatenate([values_ref[:, start : start + head_size], ones], axis=1)
        summed = jnp.dot(weights_ref[head], values, preferred_element_type=jnp.float32)
        weighted, row_sum = summed[:, :head_size], summed[:, head_size:]
        mixed[:, head * head_size : (head + 1) * head_size] = (
            weighted / jnp.maximum(row_sum, 1.0)
        ).astype(jnp.bfloat16)
        if (head + 1) % STORE_HEADS == 0 or head + 1 == heads:
            first = head // STORE_HEADS * STORE_HEADS
            part = pl.ds(first * head_size, (head + 1 - first) * head_size)
            store = pltpu.make_async_copy(mixed.at[:, part], out_hbm.at[:, part], out_sem.at[len(stores)])
            store.start()
            stores.append(store)
    for store in stores:
        store.wait()


def mix(weights, values, head_size):
    heads, tokens, _ = weights.shape
    vmem = pl.BlockSpec(memory_space=pltpu.VMEM)
    return pl.pallas_call(
        functools.partial(mix_kernel, head_size),
        out_shape=jax.ShapeDtypeStruct((tokens, heads * head_size), jnp.bfloat16),
        in_specs=[vmem, vmem],
        out_specs=pl.BlockSpec(memory_space=pl.ANY),
        scratch_shapes=[
            pltpu.VMEM((tokens, heads * head_size), jnp.bfloat16),
            pltpu.SemaphoreType.DMA((pl.cdiv(heads, STORE_HEADS),)),
        ],
        compiler_params=pltpu.CompilerParams(vmem_limit_bytes=16 * MIB),
        name="mix",
    )(weights, values)


def attend_kernel(head_size, counts_ref, range_ref, queries_ref, keys_ref, values_ref, out_ref, marks, row_mark):
    vision_rows = keys_ref.shape[0]

    @pl.when(pl.program_id(0) == 0)
    def _():
        marks[...] = token_marks(range_ref, counts_ref.shape[0], head_size)
        row_mark[...] = row_marks(counts_ref, vision_rows, head_size)

    scale = math.log2(math.e) / math.sqrt(head_size)
    kv_block = keys_ref.shape[1] // head_size
    group_width = queries_ref.shape[1] // kv_block
    ones = jnp.ones((vision_rows, head_size), jnp.bfloat16)
    for kv_head in range(kv_block):
        kv_part = pl.ds(kv_head * head_size, head_size)
        keys = jnp.concatenate([keys_ref[:, kv_part], row_mark[...]], axis=1)
        values = jnp.concatenate([values_ref[:, kv_part], ones], axis=1)
        for start in range(kv_head * group_width, (kv_head + 1) * group_width, head_size):
            head = pl.ds(start, head_size)
            marked = jnp.concatenate([queries_ref[:, head], marks[...]], axis=1)
            scores = lax.dot_general(marked, keys, (((1,), (1,)), ((), ())), preferred_element_type=jnp.float32)
            row_max = jnp.maximum(jnp.max(scores, axis=1, keepdims=True), -1e29)
            weights = jnp.exp2((scores - row_max) * scale).astype(jnp.bfloat16)
            summed = jnp.dot(weights, values, preferred_element_type=jnp.float32)
            weighted, row_sum = summed[:, :head_size], summed[:, head_size:]
            out_ref[:, head] = (weighted / jnp.maximum(row_sum, 1.0)).astype(jnp.bfloat16)


def attend(queries, keys, values, image_range, image_counts, head_size):
    tokens, query_width = queries.shape
    vision_rows, kv_width = keys.shape
    steps = math.gcd(kv_width // head_size, STEPS)
    group_width = query_width // steps
    kv_block = kv_width // steps
    return pl.pallas_call(
        functools.partial(attend_kernel, head_size),
        out_shape=jax.ShapeDtypeStruct(queries.shape, jnp.bfloat16),
        grid=(steps,),
        in_specs=[
            pl.BlockSpec(memory_space=pltpu.SMEM),
            pl.BlockSpec((2, tokens), lambda h: (0, 0)),
            pl.BlockSpec((tokens, group_width), lambda h: (0, h)),
            pl.BlockSpec((vision_rows, kv_block), lambda h: (0, h)),
            pl.BlockSpec((vision_rows, kv_block), lambda h: (0, h)),
        ],
        out_specs=pl.BlockSpec((tokens, group_width), lambda h: (0, h)),
        scratch_shapes=[
            pltpu.VMEM((tokens, head_size), jnp.bfloat16),
            pltpu.VMEM((vision_rows, head_size), jnp.bfloat16),
        ],
        name="attend",
    )(image_counts, image_range.T, queries, keys, values)


def per_device(queries, vision, w_key, w_value, key_gain, image_range, image_counts):
    head_size = key_gain.shape[0]
    tokens, query_width = queries.shape
    vision_rows = vision.shape[0] * lax.axis_size("seq")
    weight_bytes = query_width // head_size * tokens * vision_rows * 2
    fused = weight_bytes <= WEIGHTS_MAX
    extra = (image_counts, image_range.T, queries) if fused else ()
    first, values = project(vision, w_key, w_value, key_gain, extra)
    values = values.reshape(vision_rows, -1)
    if fused:
        return mix(first, values, head_size)
    return attend(queries, first.reshape(vision_rows, -1), values, image_range, image_counts, head_size)


def solution(mesh):
    placed = (
        P(("groups", "seq"), None),
        P(("groups", "seq"), None),
        P("seq", None),
        P("seq", None),
        P(),
        P(("groups", "seq"), None),
        P("groups"),
    )
    return jax.shard_map(
        per_device,
        mesh=mesh,
        in_specs=placed,
        out_specs=P(("groups", "seq"), None),
        check_vma=False,
    )
```

```python
import functools
import math

import jax
import jax.numpy as jnp
from jax import lax
from jax.experimental import pallas as pl
from jax.experimental.pallas import tpu as pltpu
from jax.sharding import PartitionSpec as P

MESH = pl.DeviceIdType.MESH
CORES = 2
STEPS = 2
STORE_HEADS = 4
ONES = 16
EARLY_HEADS = 18
LINK = jnp.bfloat16
MASKED = -1e30
MIB = 1024 * 1024
WEIGHTS_MAX = 8 * MIB


def normed_keys(raw_keys, gain):
    head_size = gain.shape[1]
    heads = []
    for start in range(0, raw_keys.shape[1], head_size):
        head = raw_keys[:, start : start + head_size]
        inverse_rms = lax.rsqrt(jnp.mean(head * head, axis=1, keepdims=True) + 1e-05)
        heads.append((head * inverse_rms * gain).astype(jnp.bfloat16))
    return jnp.concatenate(heads, axis=1)


def token_marks(range_ref, images, width):
    low_ends, high_ends = range_ref[0:1, :], range_ref[1:2, :]
    image = lax.broadcasted_iota(jnp.int32, (width, 1), 0)
    outside = (image < low_ends) | (image >= high_ends)
    marked = ((image < images) & outside) | (image == images)
    return jnp.where(marked, 1.0, 0.0).T.astype(jnp.bfloat16)


def row_marks(counts_ref, vision_rows, width):
    images = counts_ref.shape[0]
    slot_count = vision_rows // images
    index = lax.broadcasted_iota(jnp.int32, (vision_rows, width), 0)
    column = lax.broadcasted_iota(jnp.int32, (vision_rows, width), 1)
    image = jnp.zeros_like(index)
    first = jnp.zeros_like(index)
    limit = jnp.zeros_like(index) + counts_ref[0]
    for i in range(1, images):
        past = index >= i * slot_count
        image = jnp.where(past, i, image)
        first = jnp.where(past, i * slot_count, first)
        limit = jnp.where(past, counts_ref[i], limit)
    dead = index - first >= limit
    return jnp.where((column == image) | ((column == images) & dead), MASKED, 0.0).astype(jnp.bfloat16)


def project_kernel(chips, fused, *refs):
    if fused:
        vision_hbm, w_key_hbm, w_value_hbm, gain_hbm, counts_hbm, range_hbm, queries_hbm = refs[:7]
        weights_ref, values_ref = refs[7:9]
        counts_ref, range_ref, queries, marks, row_mark, extra_sem = refs[9:15]
        refs = refs[15:]
    else:
        vision_hbm, w_key_hbm, w_value_hbm, gain_hbm, keys_ref, values_ref = refs[:6]
        refs = refs[6:]
    (
        gain_ref, gain_sem, vision, columns, w_both, partial, sent, arrived, gathered,
        load_sem, weight_load_sem, weight_send_sem, weight_recv_sem, vision_send, vision_recv,
        partial_send, partial_recv, gather_send, gather_recv, forward_send, forward_recv,
    ) = refs
    me = lax.axis_index("seq")
    group = lax.axis_index("groups")
    chip, core = me // CORES, me % CORES
    depth = w_key_hbm.shape[0]
    width = CORES * depth
    rows = columns.shape[1]
    partner = (group, chip * CORES + (1 - core))
    hops = chips - 1
    peers = [lax.rem(chip + step, chips) for step in range(1, chips)]
    sources = [lax.rem(chip + chips - step, chips) for step in range(1, chips)]

    def at(chip_index):
        return (group, chip_index * CORES + core)

    load = pltpu.make_async_copy(vision_hbm, vision, load_sem)
    load.start()
    mine = pl.ds(pl.multiple_of(core * depth, depth), depth)
    weights = [w_key_hbm, w_value_hbm]
    weight_loads = [
        pltpu.make_async_copy(weights[i], w_both.at[i, mine], weight_load_sem.at[i]) for i in range(2)
    ]
    for copy in weight_loads:
        copy.start()
    gain_load = pltpu.make_async_copy(gain_hbm, gain_ref, gain_sem)
    gain_load.start()
    if fused:
        counts_load, range_load, query_load = [
            pltpu.make_async_copy(source, target, extra_sem.at[i])
            for i, (source, target) in enumerate(
                [(counts_hbm, counts_ref), (range_hbm, range_ref), (queries_hbm, queries)]
            )
        ]
        counts_load.start()
        range_load.start()
        query_load.start()

    barrier = pltpu.get_barrier_semaphore()
    for peer in peers:
        pl.semaphore_signal(barrier, inc=1, device_id=at(peer), device_id_type=MESH)
    pl.semaphore_signal(barrier, inc=1, device_id=partner, device_id_type=MESH)
    pl.semaphore_wait(barrier, chips)

    def remote(src, dst, send_sem, recv_sem, device):
        return pltpu.make_async_remote_copy(
            src_ref=src, dst_ref=dst, send_sem=send_sem, recv_sem=recv_sem,
            device_id=device, device_id_type=MESH,
        )

    load.wait()
    vision_copies = []
    for step, peer in reversed(list(enumerate(peers))):
        part = pl.ds(pl.multiple_of(peer * width, 128), width)
        copy = remote(vision.at[:, part], columns.at[step], vision_send.at[step], vision_recv.at[step], at(peer))
        copy.start()
        vision_copies.append(copy)
    for copy in weight_loads:
        copy.wait()
    weight_sends = [
        remote(w_both.at[i, mine], w_both.at[i, mine], weight_send_sem.at[i], weight_recv_sem.at[i], partner)
        for i in range(2)
    ]
    for copy in weight_sends:
        copy.start()
    columns[hops] = vision[:, pl.ds(pl.multiple_of(chip * width, 128), width)]
    gain_load.wait()
    if fused:
        counts_load.wait()
        range_load.wait()
        marks[...] = token_marks(range_ref, counts_ref.shape[0], marks.shape[1])
        row_mark[...] = row_marks(counts_ref, *row_mark.shape)
    for copy in weight_sends:
        copy.wait()

    for copy in vision_copies:
        copy.wait()

    partial_copies = ([], [])
    for i in range(2):
        left = columns[...].reshape(chips * rows, width)
        product = jnp.dot(left, w_both[i], preferred_element_type=jnp.float32).reshape(chips, rows, -1)
        sent[i] = product[:hops].astype(sent.dtype)
        partial[i] = product[hops]
        for step in range(hops):
            copy = remote(
                sent.at[i, step], arrived.at[i, step], partial_send.at[i, step], partial_recv.at[i, step],
                at(sources[step]),
            )
            copy.start()
            partial_copies[i].append(copy)

    def forward(i, source, slot):
        ref = gathered.at[i, source]
        copy = remote(ref, ref, forward_send.at[i, slot], forward_recv.at[i, slot], partner)
        copy.start()
        return copy

    gathers, forwards = [], ([], [])
    for i in range(2):
        total = partial[i]
        for step, copy in enumerate(partial_copies[i]):
            copy.wait()
            total = total + arrived[i, step].astype(jnp.float32)
        done = normed_keys(total, gain_ref[...]) if i == 0 else total.astype(jnp.bfloat16)
        gathered[i, me] = done
        ref = gathered.at[i, me]
        stream_copies = []
        for step, peer in enumerate(peers):
            copy = remote(ref, ref, gather_send.at[i, step], gather_recv.at[i, step], at(peer))
            copy.start()
            stream_copies.append(copy)
        gathers.append(stream_copies)
        forwards[i].append(forward(i, me, 0))

    def pass_on(i):
        for step in reversed(range(hops)):
            gathers[i][step].wait()
            source = sources[step] * CORES + core
            forwards[i].append(forward(i, source, step + 1))

    def settle(i):
        for copy in forwards[i]:
            copy.wait()

    pass_on(0)
    settle(0)
    if fused:
        query_load.wait()
        head_size = gain_ref.shape[1]
        heads = weights_ref.shape[0]
        group_size = heads // (gathered.shape[3] // head_size)
        scale = math.log2(math.e) / math.sqrt(head_size)

        def weigh(head):
            start = head // group_size * head_size
            keys = gathered[0, :, :, start : start + head_size].reshape(-1, head_size)
            keys = jnp.concatenate([keys, row_mark[...]], axis=1)
            marked = jnp.concatenate([queries[:, head * head_size : (head + 1) * head_size], marks[...]], axis=1)
            scores = lax.dot_general(keys, marked, (((1,), (1,)), ((), ())), preferred_element_type=jnp.float32)
            row_max = jnp.maximum(jnp.max(scores, axis=0, keepdims=True), -1e29)
            weights_ref[head] = jnp.exp2((scores - row_max) * scale).astype(jnp.bfloat16)

        early = min(EARLY_HEADS, heads)
        for head in range(early):
            weigh(head)
        pass_on(1)
        for head in range(early, heads):
            weigh(head)
    else:
        pass_on(1)
        keys_ref[...] = gathered[0]
    settle(1)
    values_ref[...] = gathered[1]


def project(vision, w_key, w_value, key_gain, extra):
    shards = lax.axis_size("seq")
    chips = shards // CORES
    rows, full = vision.shape
    depth, kv_width = w_key.shape
    head_size = key_gain.shape[0]
    fused = bool(extra)
    block = jax.ShapeDtypeStruct((shards, rows, kv_width), jnp.bfloat16)
    dma = pltpu.SemaphoreType.DMA
    hops = chips - 1
    f32, bf16 = jnp.float32, jnp.bfloat16
    hbm, vmem = pl.BlockSpec(memory_space=pltpu.HBM), pl.BlockSpec(memory_space=pltpu.VMEM)
    inputs = (vision, w_key, w_value, key_gain.reshape(1, -1), *extra)
    extra_scratch = []
    first = block
    if fused:
        tokens, query_width = extra[2].shape
        first = jax.ShapeDtypeStruct((query_width // head_size, shards * rows, tokens), bf16)
        extra_scratch = [
            pltpu.SMEM(extra[0].shape, jnp.int32),
            pltpu.VMEM(extra[1].shape, jnp.int32),
            pltpu.VMEM((tokens, query_width), bf16),
            pltpu.VMEM((tokens, head_size), bf16),
            pltpu.VMEM((shards * rows, head_size), bf16),
            dma((3,)),
        ]
    return pl.pallas_call(
        functools.partial(project_kernel, chips, fused),
        out_shape=(first, block),
        in_specs=[hbm] * len(inputs),
        out_specs=(vmem, vmem),
        scratch_shapes=[
            *extra_scratch,
            pltpu.VMEM((1, head_size), f32),
            dma,
            pltpu.VMEM((rows, full), bf16),
            pltpu.VMEM((chips, rows, CORES * depth), bf16),
            pltpu.VMEM((2, CORES * depth, kv_width), bf16),
            pltpu.VMEM((2, rows, kv_width), f32),
            pltpu.VMEM((2, hops, rows, kv_width), LINK),
            pltpu.VMEM((2, hops, rows, kv_width), LINK),
            pltpu.VMEM((2, shards, rows, kv_width), bf16),
            dma, dma((2,)), dma((2,)), dma((2,)), dma((hops,)), dma((hops,)),
            dma((2, hops)), dma((2, hops)), dma((2, hops)), dma((2, hops)), dma((2, chips)), dma((2, chips)),
        ],
        compiler_params=pltpu.CompilerParams(
            collective_id=0, has_side_effects=True, vmem_limit_bytes=24 * MIB
        ),
        name="project",
    )(*[pltpu.with_memory_space_constraint(each, pltpu.HBM) for each in inputs])


def mix_kernel(head_size, weights_ref, values_ref, out_hbm, mixed, out_sem):
    heads, vision_rows, _ = weights_ref.shape
    kv_heads = values_ref.shape[1] // head_size
    group_size = heads // kv_heads
    ones = jnp.ones((ONES, vision_rows), jnp.bfloat16)
    stores = []
    for head in range(heads):
        if head % group_size == 0:
            start = head // group_size * head_size
            values = jnp.concatenate([values_ref[:, start : start + head_size].T, ones], axis=0)
        summed = jnp.dot(values, weights_ref[head], preferred_element_type=jnp.float32)
        weighted, row_sum = summed[:head_size], summed[head_size : head_size + 1]
        mixed[:, head * head_size : (head + 1) * head_size] = (
            (weighted * (1.0 / jnp.maximum(row_sum, 1.0))).astype(jnp.bfloat16).T
        )
        if (head + 1) % STORE_HEADS == 0 or head + 1 == heads:
            first = head // STORE_HEADS * STORE_HEADS
            part = pl.ds(first * head_size, (head + 1 - first) * head_size)
            store = pltpu.make_async_copy(mixed.at[:, part], out_hbm.at[:, part], out_sem.at[len(stores)])
            store.start()
            stores.append(store)
    for store in stores:
        store.wait()


def mix(weights, values, head_size):
    heads, _, tokens = weights.shape
    vmem = pl.BlockSpec(memory_space=pltpu.VMEM)
    return pl.pallas_call(
        functools.partial(mix_kernel, head_size),
        out_shape=jax.ShapeDtypeStruct((tokens, heads * head_size), jnp.bfloat16),
        in_specs=[vmem, vmem],
        out_specs=pl.BlockSpec(memory_space=pl.ANY),
        scratch_shapes=[
            pltpu.VMEM((tokens, heads * head_size), jnp.bfloat16),
            pltpu.SemaphoreType.DMA((pl.cdiv(heads, STORE_HEADS),)),
        ],
        compiler_params=pltpu.CompilerParams(vmem_limit_bytes=16 * MIB),
        name="mix",
    )(weights, values)


def attend_kernel(head_size, counts_ref, range_ref, queries_ref, keys_ref, values_ref, out_ref, marks, row_mark):
    vision_rows = keys_ref.shape[0]

    @pl.when(pl.program_id(0) == 0)
    def _():
        marks[...] = token_marks(range_ref, counts_ref.shape[0], head_size)
        row_mark[...] = row_marks(counts_ref, vision_rows, head_size)

    scale = math.log2(math.e) / math.sqrt(head_size)
    kv_block = keys_ref.shape[1] // head_size
    group_width = queries_ref.shape[1] // kv_block
    ones = jnp.ones((vision_rows, head_size), jnp.bfloat16)
    for kv_head in range(kv_block):
        kv_part = pl.ds(kv_head * head_size, head_size)
        keys = jnp.concatenate([keys_ref[:, kv_part], row_mark[...]], axis=1)
        values = jnp.concatenate([values_ref[:, kv_part], ones], axis=1)
        for start in range(kv_head * group_width, (kv_head + 1) * group_width, head_size):
            head = pl.ds(start, head_size)
            marked = jnp.concatenate([queries_ref[:, head], marks[...]], axis=1)
            scores = lax.dot_general(marked, keys, (((1,), (1,)), ((), ())), preferred_element_type=jnp.float32)
            row_max = jnp.maximum(jnp.max(scores, axis=1, keepdims=True), -1e29)
            weights = jnp.exp2((scores - row_max) * scale).astype(jnp.bfloat16)
            summed = jnp.dot(weights, values, preferred_element_type=jnp.float32)
            weighted, row_sum = summed[:, :head_size], summed[:, head_size:]
            out_ref[:, head] = (weighted / jnp.maximum(row_sum, 1.0)).astype(jnp.bfloat16)


def attend(queries, keys, values, image_range, image_counts, head_size):
    tokens, query_width = queries.shape
    vision_rows, kv_width = keys.shape
    steps = math.gcd(kv_width // head_size, STEPS)
    group_width = query_width // steps
    kv_block = kv_width // steps
    return pl.pallas_call(
        functools.partial(attend_kernel, head_size),
        out_shape=jax.ShapeDtypeStruct(queries.shape, jnp.bfloat16),
        grid=(steps,),
        in_specs=[
            pl.BlockSpec(memory_space=pltpu.SMEM),
            pl.BlockSpec((2, tokens), lambda h: (0, 0)),
            pl.BlockSpec((tokens, group_width), lambda h: (0, h)),
            pl.BlockSpec((vision_rows, kv_block), lambda h: (0, h)),
            pl.BlockSpec((vision_rows, kv_block), lambda h: (0, h)),
        ],
        out_specs=pl.BlockSpec((tokens, group_width), lambda h: (0, h)),
        scratch_shapes=[
            pltpu.VMEM((tokens, head_size), jnp.bfloat16),
            pltpu.VMEM((vision_rows, head_size), jnp.bfloat16),
        ],
        name="attend",
    )(image_counts, image_range.T, queries, keys, values)


def per_device(queries, vision, w_key, w_value, key_gain, image_range, image_counts):
    head_size = key_gain.shape[0]
    tokens, query_width = queries.shape
    vision_rows = vision.shape[0] * lax.axis_size("seq")
    weight_bytes = query_width // head_size * tokens * vision_rows * 2
    fused = weight_bytes <= WEIGHTS_MAX
    extra = (image_counts, image_range.T, queries) if fused else ()
    first, values = project(vision, w_key, w_value, key_gain, extra)
    values = values.reshape(vision_rows, -1)
    if fused:
        return mix(first, values, head_size)
    return attend(queries, first.reshape(vision_rows, -1), values, image_range, image_counts, head_size)


def solution(mesh):
    placed = (
        P(("groups", "seq"), None),
        P(("groups", "seq"), None),
        P("seq", None),
        P("seq", None),
        P(),
        P(("groups", "seq"), None),
        P("groups"),
    )
    return jax.shard_map(
        per_device,
        mesh=mesh,
        in_specs=placed,
        out_specs=P(("groups", "seq"), None),
        check_vma=False,
    )
```

```python
import functools
import math

import jax
import jax.numpy as jnp
from jax import lax
from jax.experimental import pallas as pl
from jax.experimental.pallas import tpu as pltpu
from jax.sharding import PartitionSpec as P

MESH = pl.DeviceIdType.MESH
CORES = 2
STEPS = 2
STORE_HEADS = 4
EARLY_HEADS = 18
LINK = jnp.bfloat16
MASKED = -1e30
MIB = 1024 * 1024
WEIGHTS_MAX = 8 * MIB


def normed_keys(raw_keys, gain):
    head_size = gain.shape[1]
    heads = []
    for start in range(0, raw_keys.shape[1], head_size):
        head = raw_keys[:, start : start + head_size]
        inverse_rms = lax.rsqrt(jnp.mean(head * head, axis=1, keepdims=True) + 1e-05)
        heads.append((head * inverse_rms * gain).astype(jnp.bfloat16))
    return jnp.concatenate(heads, axis=1)


def token_marks(range_ref, images, width):
    low_ends, high_ends = range_ref[0:1, :], range_ref[1:2, :]
    image = lax.broadcasted_iota(jnp.int32, (width, 1), 0)
    outside = (image < low_ends) | (image >= high_ends)
    marked = ((image < images) & outside) | (image == images)
    return jnp.where(marked, 1.0, 0.0).T.astype(jnp.bfloat16)


def row_marks(counts_ref, vision_rows, width):
    images = counts_ref.shape[0]
    slot_count = vision_rows // images
    index = lax.broadcasted_iota(jnp.int32, (vision_rows, width), 0)
    column = lax.broadcasted_iota(jnp.int32, (vision_rows, width), 1)
    image = jnp.zeros_like(index)
    first = jnp.zeros_like(index)
    limit = jnp.zeros_like(index) + counts_ref[0]
    for i in range(1, images):
        past = index >= i * slot_count
        image = jnp.where(past, i, image)
        first = jnp.where(past, i * slot_count, first)
        limit = jnp.where(past, counts_ref[i], limit)
    dead = index - first >= limit
    return jnp.where((column == image) | ((column == images) & dead), MASKED, 0.0).astype(jnp.bfloat16)


def project_kernel(chips, fused, *refs):
    if fused:
        vision_hbm, w_key_hbm, w_value_hbm, gain_hbm, counts_hbm, range_hbm, queries_hbm = refs[:7]
        weights_ref, values_ref = refs[7:9]
        counts_ref, range_ref, queries, marks, row_mark, extra_sem = refs[9:15]
        refs = refs[15:]
    else:
        vision_hbm, w_key_hbm, w_value_hbm, gain_hbm, keys_ref, values_ref = refs[:6]
        refs = refs[6:]
    (
        gain_ref, gain_sem, vision, columns, w_both, partial, sent, arrived, gathered,
        load_sem, weight_load_sem, weight_send_sem, weight_recv_sem, vision_send, vision_recv,
        partial_send, partial_recv, gather_send, gather_recv, forward_send, forward_recv,
    ) = refs
    me = lax.axis_index("seq")
    group = lax.axis_index("groups")
    chip, core = me // CORES, me % CORES
    depth = w_key_hbm.shape[0]
    width = CORES * depth
    rows = columns.shape[1]
    partner = (group, chip * CORES + (1 - core))
    hops = chips - 1
    peers = [lax.rem(chip + step, chips) for step in range(1, chips)]
    sources = [lax.rem(chip + chips - step, chips) for step in range(1, chips)]

    def at(chip_index):
        return (group, chip_index * CORES + core)

    load = pltpu.make_async_copy(vision_hbm, vision, load_sem)
    load.start()
    mine = pl.ds(pl.multiple_of(core * depth, depth), depth)
    weights = [w_key_hbm, w_value_hbm]
    weight_loads = [
        pltpu.make_async_copy(weights[i], w_both.at[i, mine], weight_load_sem.at[i]) for i in range(2)
    ]
    for copy in weight_loads:
        copy.start()
    gain_load = pltpu.make_async_copy(gain_hbm, gain_ref, gain_sem)
    gain_load.start()
    if fused:
        counts_load, range_load, query_load = [
            pltpu.make_async_copy(source, target, extra_sem.at[i])
            for i, (source, target) in enumerate(
                [(counts_hbm, counts_ref), (range_hbm, range_ref), (queries_hbm, queries)]
            )
        ]
        counts_load.start()
        range_load.start()
        query_load.start()

    barrier = pltpu.get_barrier_semaphore()
    for peer in peers:
        pl.semaphore_signal(barrier, inc=1, device_id=at(peer), device_id_type=MESH)
    pl.semaphore_signal(barrier, inc=1, device_id=partner, device_id_type=MESH)
    pl.semaphore_wait(barrier, chips)

    def remote(src, dst, send_sem, recv_sem, device):
        return pltpu.make_async_remote_copy(
            src_ref=src, dst_ref=dst, send_sem=send_sem, recv_sem=recv_sem,
            device_id=device, device_id_type=MESH,
        )

    load.wait()
    vision_copies = []
    for step, peer in reversed(list(enumerate(peers))):
        part = pl.ds(pl.multiple_of(peer * width, 128), width)
        copy = remote(vision.at[:, part], columns.at[step], vision_send.at[step], vision_recv.at[step], at(peer))
        copy.start()
        vision_copies.append(copy)
    for copy in weight_loads:
        copy.wait()
    weight_sends = [
        remote(w_both.at[i, mine], w_both.at[i, mine], weight_send_sem.at[i], weight_recv_sem.at[i], partner)
        for i in range(2)
    ]
    for copy in weight_sends:
        copy.start()
    columns[hops] = vision[:, pl.ds(pl.multiple_of(chip * width, 128), width)]
    gain_load.wait()
    if fused:
        counts_load.wait()
        range_load.wait()
        marks[...] = token_marks(range_ref, counts_ref.shape[0], marks.shape[1])
        row_mark[...] = row_marks(counts_ref, *row_mark.shape)
    for copy in weight_sends:
        copy.wait()

    for copy in vision_copies:
        copy.wait()

    partial_copies = ([], [])
    for i in range(2):
        left = columns[...].reshape(chips * rows, width)
        product = jnp.dot(left, w_both[i], preferred_element_type=jnp.float32).reshape(chips, rows, -1)
        sent[i] = product[:hops].astype(sent.dtype)
        partial[i] = product[hops]
        for step in range(hops):
            copy = remote(
                sent.at[i, step], arrived.at[i, step], partial_send.at[i, step], partial_recv.at[i, step],
                at(sources[step]),
            )
            copy.start()
            partial_copies[i].append(copy)

    def forward(i, source, slot):
        ref = gathered.at[i, source]
        copy = remote(ref, ref, forward_send.at[i, slot], forward_recv.at[i, slot], partner)
        copy.start()
        return copy

    gathers, forwards = [], ([], [])
    for i in range(2):
        total = partial[i]
        for step, copy in enumerate(partial_copies[i]):
            copy.wait()
            total = total + arrived[i, step].astype(jnp.float32)
        done = normed_keys(total, gain_ref[...]) if i == 0 else total.astype(jnp.bfloat16)
        gathered[i, me] = done
        ref = gathered.at[i, me]
        stream_copies = []
        for step, peer in enumerate(peers):
            copy = remote(ref, ref, gather_send.at[i, step], gather_recv.at[i, step], at(peer))
            copy.start()
            stream_copies.append(copy)
        gathers.append(stream_copies)
        forwards[i].append(forward(i, me, 0))

    def pass_on(i):
        for step in reversed(range(hops)):
            gathers[i][step].wait()
            source = sources[step] * CORES + core
            forwards[i].append(forward(i, source, step + 1))

    def settle(i):
        for copy in forwards[i]:
            copy.wait()

    pass_on(0)
    settle(0)
    if fused:
        query_load.wait()
        head_size = gain_ref.shape[1]
        heads = weights_ref.shape[0]
        group_size = heads // (gathered.shape[3] // head_size)
        scale = math.log2(math.e) / math.sqrt(head_size)

        def weigh(head):
            start = head // group_size * head_size
            keys = gathered[0, :, :, start : start + head_size].reshape(-1, head_size)
            keys = jnp.concatenate([keys, row_mark[...]], axis=1)
            marked = jnp.concatenate([queries[:, head * head_size : (head + 1) * head_size], marks[...]], axis=1)
            scores = lax.dot_general(marked, keys, (((1,), (1,)), ((), ())), preferred_element_type=jnp.float32)
            row_max = jnp.maximum(jnp.max(scores, axis=1, keepdims=True), -1e29)
            weights_ref[head] = jnp.exp2((scores - row_max) * scale).astype(jnp.bfloat16)

        early = min(EARLY_HEADS, heads)
        for head in range(early):
            weigh(head)
        pass_on(1)
        for head in range(early, heads):
            weigh(head)
    else:
        pass_on(1)
        keys_ref[...] = gathered[0]
    settle(1)
    values_ref[...] = gathered[1]


def project(vision, w_key, w_value, key_gain, extra):
    shards = lax.axis_size("seq")
    chips = shards // CORES
    rows, full = vision.shape
    depth, kv_width = w_key.shape
    head_size = key_gain.shape[0]
    fused = bool(extra)
    block = jax.ShapeDtypeStruct((shards, rows, kv_width), jnp.bfloat16)
    dma = pltpu.SemaphoreType.DMA
    hops = chips - 1
    f32, bf16 = jnp.float32, jnp.bfloat16
    hbm, vmem = pl.BlockSpec(memory_space=pltpu.HBM), pl.BlockSpec(memory_space=pltpu.VMEM)
    inputs = (vision, w_key, w_value, key_gain.reshape(1, -1), *extra)
    extra_scratch = []
    first = block
    if fused:
        tokens, query_width = extra[2].shape
        first = jax.ShapeDtypeStruct((query_width // head_size, tokens, shards * rows), bf16)
        extra_scratch = [
            pltpu.SMEM(extra[0].shape, jnp.int32),
            pltpu.VMEM(extra[1].shape, jnp.int32),
            pltpu.VMEM((tokens, query_width), bf16),
            pltpu.VMEM((tokens, head_size), bf16),
            pltpu.VMEM((shards * rows, head_size), bf16),
            dma((3,)),
        ]
    return pl.pallas_call(
        functools.partial(project_kernel, chips, fused),
        out_shape=(first, block),
        in_specs=[hbm] * len(inputs),
        out_specs=(vmem, vmem),
        scratch_shapes=[
            *extra_scratch,
            pltpu.VMEM((1, head_size), f32),
            dma,
            pltpu.VMEM((rows, full), bf16),
            pltpu.VMEM((chips, rows, CORES * depth), bf16),
            pltpu.VMEM((2, CORES * depth, kv_width), bf16),
            pltpu.VMEM((2, rows, kv_width), f32),
            pltpu.VMEM((2, hops, rows, kv_width), LINK),
            pltpu.VMEM((2, hops, rows, kv_width), LINK),
            pltpu.VMEM((2, shards, rows, kv_width), bf16),
            dma, dma((2,)), dma((2,)), dma((2,)), dma((hops,)), dma((hops,)),
            dma((2, hops)), dma((2, hops)), dma((2, hops)), dma((2, hops)), dma((2, chips)), dma((2, chips)),
        ],
        compiler_params=pltpu.CompilerParams(
            collective_id=0, has_side_effects=True, vmem_limit_bytes=24 * MIB
        ),
        name="project",
    )(*[pltpu.with_memory_space_constraint(each, pltpu.HBM) for each in inputs])


def mix_kernel(head_size, weights_ref, values_ref, out_hbm, mixed, out_sem):
    heads, _, vision_rows = weights_ref.shape
    kv_heads = values_ref.shape[1] // head_size
    group_size = heads // kv_heads
    ones = jnp.ones((vision_rows, head_size), jnp.bfloat16)
    stores = []
    for head in range(heads):
        start = head // group_size * head_size
        values = jnp.concatenate([values_ref[:, start : start + head_size], ones], axis=1)
        summed = jnp.dot(weights_ref[head], values, preferred_element_type=jnp.float32)
        weighted, row_sum = summed[:, :head_size], summed[:, head_size:]
        mixed[:, head * head_size : (head + 1) * head_size] = (
            weighted / jnp.maximum(row_sum, 1.0)
        ).astype(jnp.bfloat16)
        if (head + 1) % STORE_HEADS == 0 or head + 1 == heads:
            first = head // STORE_HEADS * STORE_HEADS
            part = pl.ds(first * head_size, (head + 1 - first) * head_size)
            store = pltpu.make_async_copy(mixed.at[:, part], out_hbm.at[:, part], out_sem.at[len(stores)])
            store.start()
            stores.append(store)
    for store in stores:
        store.wait()


def mix(weights, values, head_size):
    heads, tokens, _ = weights.shape
    vmem = pl.BlockSpec(memory_space=pltpu.VMEM)
    return pl.pallas_call(
        functools.partial(mix_kernel, head_size),
        out_shape=jax.ShapeDtypeStruct((tokens, heads * head_size), jnp.bfloat16),
        in_specs=[vmem, vmem],
        out_specs=pl.BlockSpec(memory_space=pl.ANY),
        scratch_shapes=[
            pltpu.VMEM((tokens, heads * head_size), jnp.bfloat16),
            pltpu.SemaphoreType.DMA((pl.cdiv(heads, STORE_HEADS),)),
        ],
        compiler_params=pltpu.CompilerParams(vmem_limit_bytes=16 * MIB),
        name="mix",
    )(weights, values)


def attend_kernel(head_size, counts_ref, range_ref, queries_ref, keys_ref, values_ref, out_ref, marks, row_mark):
    vision_rows = keys_ref.shape[0]

    @pl.when(pl.program_id(0) == 0)
    def _():
        marks[...] = token_marks(range_ref, counts_ref.shape[0], head_size)
        row_mark[...] = row_marks(counts_ref, vision_rows, head_size)

    scale = math.log2(math.e) / math.sqrt(head_size)
    kv_block = keys_ref.shape[1] // head_size
    group_width = queries_ref.shape[1] // kv_block
    ones = jnp.ones((vision_rows, head_size), jnp.bfloat16)
    for kv_head in range(kv_block):
        kv_part = pl.ds(kv_head * head_size, head_size)
        keys = jnp.concatenate([keys_ref[:, kv_part], row_mark[...]], axis=1)
        values = jnp.concatenate([values_ref[:, kv_part], ones], axis=1)
        for start in range(kv_head * group_width, (kv_head + 1) * group_width, head_size):
            head = pl.ds(start, head_size)
            marked = jnp.concatenate([queries_ref[:, head], marks[...]], axis=1)
            scores = lax.dot_general(marked, keys, (((1,), (1,)), ((), ())), preferred_element_type=jnp.float32)
            row_max = jnp.maximum(jnp.max(scores, axis=1, keepdims=True), -1e29)
            weights = jnp.exp2((scores - row_max) * scale).astype(jnp.bfloat16)
            summed = jnp.dot(weights, values, preferred_element_type=jnp.float32)
            weighted, row_sum = summed[:, :head_size], summed[:, head_size:]
            out_ref[:, head] = (weighted / jnp.maximum(row_sum, 1.0)).astype(jnp.bfloat16)


def attend(queries, keys, values, image_range, image_counts, head_size):
    tokens, query_width = queries.shape
    vision_rows, kv_width = keys.shape
    steps = math.gcd(kv_width // head_size, STEPS)
    group_width = query_width // steps
    kv_block = kv_width // steps
    return pl.pallas_call(
        functools.partial(attend_kernel, head_size),
        out_shape=jax.ShapeDtypeStruct(queries.shape, jnp.bfloat16),
        grid=(steps,),
        in_specs=[
            pl.BlockSpec(memory_space=pltpu.SMEM),
            pl.BlockSpec((2, tokens), lambda h: (0, 0)),
            pl.BlockSpec((tokens, group_width), lambda h: (0, h)),
            pl.BlockSpec((vision_rows, kv_block), lambda h: (0, h)),
            pl.BlockSpec((vision_rows, kv_block), lambda h: (0, h)),
        ],
        out_specs=pl.BlockSpec((tokens, group_width), lambda h: (0, h)),
        scratch_shapes=[
            pltpu.VMEM((tokens, head_size), jnp.bfloat16),
            pltpu.VMEM((vision_rows, head_size), jnp.bfloat16),
        ],
        name="attend",
    )(image_counts, image_range.T, queries, keys, values)


def per_device(queries, vision, w_key, w_value, key_gain, image_range, image_counts):
    head_size = key_gain.shape[0]
    tokens, query_width = queries.shape
    vision_rows = vision.shape[0] * lax.axis_size("seq")
    weight_bytes = query_width // head_size * tokens * vision_rows * 2
    fused = weight_bytes <= WEIGHTS_MAX
    extra = (image_counts, image_range.T, queries) if fused else ()
    first, values = project(vision, w_key, w_value, key_gain, extra)
    values = values.reshape(vision_rows, -1)
    if fused:
        return mix(first, values, head_size)
    return attend(queries, first.reshape(vision_rows, -1), values, image_range, image_counts, head_size)


def solution(mesh):
    placed = (
        P(("groups", "seq"), None),
        P(("groups", "seq"), None),
        P("seq", None),
        P("seq", None),
        P(),
        P(("groups", "seq"), None),
        P("groups"),
    )
    return jax.shard_map(
        per_device,
        mesh=mesh,
        in_specs=placed,
        out_specs=P(("groups", "seq"), None),
        check_vma=False,
    )
```
